32 devices in a mesh: seq: 8 (over z, x), mp: 4 (over y, core).
Axes of the slice: x: 2, y: 2, z: 4, core: 2. Of those that a mesh axis runs over, the one named last changes fastest.
Arguments:
- layer_in: bfloat16 [6144, 2560], P('seq'), may hold values from -6 to 6
- ssm_input: bfloat16 [6144, 5120], P('seq', 'mp'), may hold values from -6 to 6
- b_matrix: bfloat16 [6144, 128], P('seq'), may hold values from -1.796875 to 1.796875
- c_matrix: bfloat16 [6144, 128], P('seq'), may hold values from -1.796875 to 1.796875
- dt_raw: float32 [6144, 80], P('seq', 'mp'), may hold values from -2.8 to 2.8
- dt_bias: float32 [80], P('mp'), may hold values from -7 to 0
- a_log: float32 [80], P('mp'), may hold values from -8 to 3
- d_skip: float32 [80], P('mp'), may hold values from 0.5 to 1.5
- grad_out: bfloat16 [6144, 5120], P('seq', 'mp'), may hold values from -1 to 1
Outputs:
- grad_wx: float32 [2560, 5120], P('seq', 'mp')
- grad_wbc: float32 [2560, 256], P('seq', 'mp')
- grad_alog: float32 [80], P('mp')
- grad_dtbias: float32 [80], P('mp')
- grad_dskip: float32 [80], P('mp')
The draws below stay inside these ranges and needn't reach their ends.
All inputs are finite; a program needn't handle non-finite values.
Results may differ from the reference program's by a relative error of at most 0.0063.
Values sent between devices are 32-bit elements; how exact they have to be, the bound alone decides.
A program may use at most 192 MiB of HBM per device.

```python
import math
from functools import partial
import jax
import jax.numpy as jnp
from jax import lax

D = 2560
HEADS = 80
HEAD_DIM = 64
STATE = 128
GROUP = 256
TOK_DEV = 768
TOKENS = 6144
N_SEQ = 8


def draw_dt_bias(key, part):
    centre = -0.5 * jnp.log(jnp.float32(TOKENS))
    offset = jax.random.uniform(key, (HEADS,), jnp.float32, -0.5, 0.5)
    return centre + offset


def draw_a_log(key, part):
    key_pick = jax.random.fold_in(key, 11)
    key_slow = jax.random.fold_in(key, 12)
    key_fast = jax.random.fold_in(key, 13)
    seq_root = jnp.sqrt(jnp.float32(TOKENS))
    is_slow = jax.random.bernoulli(key_pick, 0.5, (HEADS,))
    slow_rate = jnp.exp(jax.random.uniform(key_slow, (HEADS,), jnp.float32, math.log(0.15), 0.0)) / seq_root
    fast_rate = seq_root / (1.28 * jax.random.uniform(key_fast, (HEADS,), jnp.float32, 30.0, 50.0))
    return jnp.log(jnp.where(is_slow, slow_rate, fast_rate))


def draw_grad_out(key, part):
    key_main = jax.random.fold_in(key, 21)
    row_width = HEADS * HEAD_DIM
    position = jnp.arange(TOKENS, dtype=jnp.float32)[:, None]
    ramp_scale = (0.5 + 1.5 * position / TOKENS) / jnp.sqrt(jnp.float32(TOKENS))
    noise_field = jnp.clip(jax.random.normal(key_main, (TOKENS, row_width), jnp.float32), -4.0, 4.0)
    return (noise_field * ramp_scale).astype(jnp.bfloat16)


def level_of(stream_key, dims, cuts, low, top_value):
    def one(axis_at, shards_of):
        heights = jax.random.uniform(jax.random.fold_in(jax.random.fold_in(stream_key, 6), axis_at), (shards_of,), jnp.float32, low / len(cuts), top_value / len(cuts))
        return jnp.repeat(jnp.exp(heights), dims[axis_at] // shards_of).reshape((-1,) + (1,) * (len(dims) - axis_at - 1))

    gain = one(*cuts[0])
    for cut in cuts[1:]:
        gain = gain * one(*cut)
    return gain


def bell_draw(rng, extent, width, bound, split=(), held_as=jnp.bfloat16):
    values = jax.random.normal(rng, extent, jnp.float32) * width
    if len(split) > 0:
        values = level_of(rng, extent, split, -0.22, 0.18) * values
    return jnp.clip(values, min=-bound, max=bound).astype(held_as)


def setup_inputs(seed: int = 0) -> dict:
    splits = jax.random.split(jax.random.key(seed), 10)
    return {
        "layer_in": bell_draw(splits[0], (TOKENS, D), 1.0, 6.0, ((0, 8),)),
        "ssm_input": bell_draw(splits[1], (TOKENS, HEADS * HEAD_DIM), 1.0, 6.0, ((0, 8), (1, 4))),
        "b_matrix": bell_draw(splits[2], (TOKENS, STATE), 0.3, 1.796875, ((0, 8),)),
        "c_matrix": bell_draw(splits[3], (TOKENS, STATE), 0.3, 1.796875, ((0, 8),)),
        "dt_raw": bell_draw(splits[4], (TOKENS, HEADS), 0.7, 2.8, ((0, 8), (1, 4)), jnp.float32),
        "dt_bias": draw_dt_bias(jax.random.fold_in(splits[9], 71), 0),
        "a_log": draw_a_log(jax.random.fold_in(splits[9], 71), 0),
        "d_skip": jnp.clip(0.5 + 1.0 * jax.random.uniform(splits[7], (HEADS,), jnp.float32) ** level_of(splits[7], (HEADS,), ((0, 4),), -0.2, 0.2), 0.5, 1.5),
        "grad_out": draw_grad_out(jax.random.fold_in(splits[9], 71), 0),
    }


def contract(form, left, right):
    return jnp.einsum(form, left.astype(jnp.float32), right.astype(jnp.float32), precision=lax.Precision.HIGHEST)


def matmul(left, right):
    return jnp.dot(left, right, preferred_element_type=jnp.float32)


def inner_first(left, right):
    return jnp.dot(left.T, right, preferred_element_type=jnp.float32)


def inner_last(left, right):
    return jnp.dot(left, right.T, preferred_element_type=jnp.float32)


def reverse_sum(values):
    return jnp.flip(jnp.cumsum(jnp.flip(values, 0), axis=0), 0)


def exclusive_sum(values):
    return jnp.cumsum(values, axis=0) - values


def head_rates(dt_raw, dt_bias, a_log):
    shifted = dt_raw + dt_bias[None, :]
    dt_step = jax.nn.softplus(shifted)
    gate_slope = jax.nn.sigmoid(shifted)
    decay_rate = -jnp.exp(a_log)
    return dt_step, gate_slope, decay_rate, dt_step * decay_rate[None, :]


def block_states(ssm_input, grad_out, b_matrix, c_matrix, dt_step, log_step):
    tok_count, head_count = dt_step.shape
    head_dim = ssm_input.shape[1] // head_count
    state_width = b_matrix.shape[1]
    groups = tok_count // GROUP
    within = jnp.cumsum(log_step.reshape(groups, GROUP, head_count), axis=1)
    totals = within[:, -1, :]
    group_steps = dt_step.reshape(groups, GROUP, head_count)
    x_four = ssm_input.reshape(groups, GROUP, head_count, head_dim)
    dy_four = grad_out.reshape(groups, GROUP, head_count, head_dim)
    x_scaled = (x_four * (group_steps * jnp.exp(totals[:, None, :] - within))[..., None]).astype(jnp.bfloat16)
    y_scaled = (dy_four * jnp.exp(within)[..., None]).astype(jnp.bfloat16)
    b_three = b_matrix.reshape(groups, GROUP, state_width)
    c_three = c_matrix.reshape(groups, GROUP, state_width)
    state_parts = contract("kqhp,kqn->khpn", x_scaled, b_three)
    grad_parts = contract("kqhp,kqn->khpn", y_scaled, c_three)
    carry_state = jnp.zeros((head_count, head_dim, state_width), jnp.float32)
    starts = []
    for group_id in range(groups):
        starts.append(carry_state)
        carry_state = jnp.exp(totals[group_id])[:, None, None] * carry_state + state_parts[group_id]
    carry_grad = jnp.zeros((head_count, head_dim, state_width), jnp.float32)
    end_grads = [carry_grad] * groups
    for group_id in range(groups - 1, -1, -1):
        end_grads[group_id] = carry_grad
        carry_grad = grad_parts[group_id] + jnp.exp(totals[group_id])[:, None, None] * carry_grad
    cumulative = jnp.cumsum(log_step, axis=0)
    block_decay = jnp.exp(cumulative[-1])
    packed = (within, totals, x_scaled, y_scaled, jnp.stack(starts), jnp.stack(end_grads), cumulative)
    return block_decay, carry_state, carry_grad, packed


def one_group(d_skip, group_item):
    x_c, dy_c, b_c, c_c, dt_c, within_c, total_c, start_c, end_c, xw_c, yw_c = group_item
    size_q = x_c.shape[0]
    state_width = b_c.shape[1]
    cross_bc = inner_last(c_c, b_c)
    positions = jnp.arange(size_q)
    lower_mask = positions[:, None] >= positions[None, :]
    strict = positions[:, None] > positions[None, :]
    lagged = within_c.T[:, :, None] - within_c.T[:, None, :]
    decayed = jnp.where(lower_mask[None], jnp.exp(jnp.where(lower_mask[None], lagged, 0.0)), 0.0)
    mix_matrix = (cross_bc[None] * decayed).astype(jnp.bfloat16)
    gb_intra = contract("hrs,rhp->shp", mix_matrix, dy_c)
    paired = contract("rhp,shp->hrs", dy_c, x_c) * decayed
    paired_dt = paired * dt_c.T[:, None, :]
    mixed_sum = jnp.sum(paired_dt, axis=0).astype(jnp.bfloat16)
    box_terms = jnp.where(strict[None], cross_bc[None] * paired_dt, 0.0)
    box_flow = jnp.sum(box_terms, axis=1) - jnp.sum(box_terms, axis=2)
    da_intra = (jnp.cumsum(box_flow, axis=1) - box_flow).T
    start_low = start_c.astype(jnp.bfloat16)
    end_low = end_c.astype(jnp.bfloat16)
    y_start = contract("hpn,qn->qhp", start_low, c_c) * jnp.exp(within_c)[:, :, None]
    gb_end = contract("hpn,qn->qhp", end_low, b_c) * jnp.exp(total_c[None, :] - within_c)[:, :, None]
    gb_local = gb_intra + gb_end
    dx_local = (dt_c[:, :, None] * gb_local + d_skip[None, :, None] * dy_c).astype(jnp.bfloat16)
    x_wide = x_c.astype(jnp.float32)
    dy_wide = dy_c.astype(jnp.float32)
    x_gb = jnp.sum(x_wide * gb_local, axis=2)
    backward_part = jnp.sum(dy_wide * y_start, axis=2)
    forward_part = dt_c * jnp.sum(x_wide * gb_end, axis=2)
    meeting = jnp.exp(total_c) * jnp.sum(end_c * start_c, axis=(1, 2))
    da_local = da_intra + reverse_sum(backward_part) + exclusive_sum(forward_part) + meeting[None, :]
    dc_part = matmul(mixed_sum, b_c) + matmul(yw_c.reshape(size_q, -1), start_low.reshape(-1, state_width))
    db_part = inner_first(mixed_sum, c_c) + matmul(xw_c.reshape(size_q, -1), end_low.reshape(-1, state_width))
    return dx_local, jnp.concatenate([db_part, dc_part], axis=1), x_gb, da_local


def group_local(ssm_input, grad_out, b_matrix, c_matrix, dt_step, d_skip, packed):
    within, totals, x_scaled, y_scaled, starts, end_grads, cumulative = packed
    tok_count, head_count = dt_step.shape
    groups = within.shape[0]
    head_dim = ssm_input.shape[1] // head_count
    group_items = (ssm_input.reshape(groups, GROUP, head_count, head_dim),
                   grad_out.reshape(groups, GROUP, head_count, head_dim),
                   b_matrix.reshape(groups, GROUP, -1), c_matrix.reshape(groups, GROUP, -1),
                   dt_step.reshape(groups, GROUP, head_count), within, totals, starts, end_grads,
                   x_scaled, y_scaled)
    dx_local, dbc_local, x_gb, da_local = lax.map(partial(one_group, d_skip), group_items)
    return (dx_local.reshape(tok_count, -1), dbc_local.reshape(tok_count, -1),
            x_gb.reshape(tok_count, head_count), da_local.reshape(tok_count, head_count))


def device_terms(ssm_input, grad_out, b_matrix, c_matrix, dt_step, cumulative, state_in, grad_in):
    tok_count, head_count = dt_step.shape
    head_dim = ssm_input.shape[1] // head_count
    state_width = b_matrix.shape[1]
    block_end = cumulative[-1]
    state_low = state_in.astype(jnp.bfloat16)
    grad_low = grad_in.astype(jnp.bfloat16)
    rise_factor = jnp.exp(cumulative)
    fall_factor = jnp.exp(block_end[None, :] - cumulative)
    x_three = ssm_input.reshape(tok_count, head_count, head_dim)
    dy_three = grad_out.reshape(tok_count, head_count, head_dim)
    y_dev = contract("hpn,tn->thp", state_low, c_matrix) * rise_factor[:, :, None]
    gb_dev = contract("hpn,tn->thp", grad_low, b_matrix) * fall_factor[:, :, None]
    dx_carry = (dt_step[:, :, None] * gb_dev).astype(jnp.bfloat16).reshape(tok_count, -1)
    x_gb = jnp.sum(x_three.astype(jnp.float32) * gb_dev, axis=2)
    backward_part = jnp.sum(dy_three.astype(jnp.float32) * y_dev, axis=2)
    forward_part = dt_step * x_gb
    meeting = jnp.exp(block_end) * jnp.sum(grad_in * state_in, axis=(1, 2))
    da_dev = reverse_sum(backward_part) + exclusive_sum(forward_part) + meeting[None, :]
    y_rise = (dy_three * rise_factor[:, :, None]).astype(jnp.bfloat16).reshape(tok_count, -1)
    x_fall = (x_three * (dt_step * fall_factor)[:, :, None]).astype(jnp.bfloat16).reshape(tok_count, -1)
    dc_dev = matmul(y_rise, state_low.reshape(-1, state_width))
    db_dev = matmul(x_fall, grad_low.reshape(-1, state_width))
    return dx_carry, jnp.concatenate([db_dev, dc_dev], axis=1), x_gb, da_dev


def head_totals(ssm_input, grad_out, dt_step, gate_slope, decay_rate, x_gb, da_all):
    tok_count, head_count = dt_step.shape
    derivative = x_gb + decay_rate[None, :] * da_all
    skip_terms = jnp.sum((ssm_input.astype(jnp.float32) * grad_out.astype(jnp.float32)).reshape(tok_count, head_count, -1), axis=2)
    return jnp.sum(dt_step * da_all, axis=0), jnp.sum(gate_slope * derivative, axis=0), jnp.sum(skip_terms, axis=0)


def reference(layer_in, ssm_input, b_matrix, c_matrix, dt_raw, dt_bias, a_log, d_skip, grad_out):
    dt_step, gate_slope, decay_rate, log_step = head_rates(dt_raw, dt_bias, a_log)

    def block_piece(array, block_id):
        return lax.dynamic_slice_in_dim(array, (block_id * TOK_DEV).astype(jnp.int32), TOK_DEV, 0)

    def pieces(block_id):
        return tuple(block_piece(array, block_id) for array in (ssm_input, grad_out, b_matrix, c_matrix, dt_step, log_step))

    def summary(block_id):
        block_decay, block_state, block_grad, packed = block_states(*pieces(block_id))
        return block_decay, block_state, block_grad

    block_ids = jnp.arange(N_SEQ, dtype=jnp.int32)
    decays, states, grads = lax.map(summary, block_ids)

    def forward(running_state, entry):
        return entry[0][:, None, None] * running_state + entry[1], running_state

    def backward(running_state, entry):
        return entry[1] + entry[0][:, None, None] * running_state, running_state

    zero_state = jnp.zeros_like(states[0])
    final_state, states_in = lax.scan(forward, zero_state, (decays, states))
    first_grad, grads_in = lax.scan(backward, zero_state, (decays, grads), reverse=True)

    def accumulate(running, block_id):
        wx_total, wbc_total, rate_total, bias_total, skip_total = running
        x_blk, dy_blk, b_blk, c_blk, dt_blk, log_blk = pieces(block_id)
        block_decay, block_state, block_grad, packed = block_states(x_blk, dy_blk, b_blk, c_blk, dt_blk, log_blk)
        local_part = group_local(x_blk, dy_blk, b_blk, c_blk, dt_blk, d_skip, packed)
        carried = device_terms(x_blk, dy_blk, b_blk, c_blk, dt_blk, packed[6], states_in[block_id], grads_in[block_id])
        u_blk = block_piece(layer_in, block_id)
        wx_total = wx_total + (inner_first(u_blk, local_part[0]) + inner_first(u_blk, carried[0]))
        dbc_low = (local_part[1] + carried[1]).astype(jnp.bfloat16)
        wbc_total = wbc_total + inner_first(u_blk, dbc_low)
        slope_blk = block_piece(gate_slope, block_id)
        rate_part, bias_part, skip_part = head_totals(x_blk, dy_blk, dt_blk, slope_blk, decay_rate,
                                                      local_part[2] + carried[2], local_part[3] + carried[3])
        return (wx_total, wbc_total, rate_total + rate_part, bias_total + bias_part, skip_total + skip_part), None

    start = (jnp.zeros((D, HEADS * HEAD_DIM), jnp.float32), jnp.zeros((D, 2 * STATE), jnp.float32),
             jnp.zeros((HEADS,), jnp.float32), jnp.zeros((HEADS,), jnp.float32), jnp.zeros((HEADS,), jnp.float32))
    totals_out, unused = lax.scan(accumulate, start, block_ids)
    grad_wx, grad_wbc, rate_sum, bias_sum, skip_sum = totals_out
    return grad_wx, grad_wbc, decay_rate * rate_sum, bias_sum, skip_sum
```

```python
from functools import partial

import jax
import jax.numpy as jnp
from jax import lax
from jax.experimental import pallas as pl
from jax.experimental.pallas import tpu as pltpu
from jax.sharding import PartitionSpec as P

GROUP = 256
HALF = 128
ROWS = 16
LOG2E = 1.4426950408889634
HIGH = lax.Precision.HIGHEST
MESH = pl.DeviceIdType.MESH
F32 = jnp.float32
BF16 = jnp.bfloat16
L2, DT, EL, FE, SL, UPD, UPS, AFD, AFS, XB, YB = range(11)


def nn(a, b, precision=None):
    return lax.dot_general(
        a, b, (((1,), (0,)), ((), ())), precision=precision, preferred_element_type=F32
    )


def nt(a, b):
    return lax.dot_general(a, b, (((1,), (1,)), ((), ())), preferred_element_type=F32)


def tn(a, b):
    return lax.dot_general(a, b, (((0,), (0,)), ((), ())), preferred_element_type=F32)


def pair_wide(cols, row, first):
    low = cols[:, row : row + 1]
    high = cols[:, ROWS + row : ROWS + row + 1]
    return jnp.where(first, low, high)


def states_kernel(x_ref, dy_ref, b_ref, c_ref, tab_ref, s_ref, g_ref):
    cols = tab_ref[0].T
    first = lax.broadcasted_iota(jnp.int32, (1, 128), 1) < 64
    xb = (x_ref[...].astype(F32) * pair_wide(cols, XB, first)).astype(BF16)
    yb = (dy_ref[...].astype(F32) * pair_wide(cols, YB, first)).astype(BF16)
    s_ref[0] = tn(b_ref[...], xb)
    g_ref[0] = tn(c_ref[...], yb)


def group_kernel(
    groups, x_ref, dy_ref, b_ref, c_ref, tab_ref, skip_ref, sin_ref, gin_ref,
    dx_ref, dbc_ref, sums_ref, small_ref, cross, vt, starts, ends,
):
    pair = pl.program_id(0)
    state = b_ref.shape[1]
    first = lax.broadcasted_iota(jnp.int32, (1, 128), 1) < 64

    @pl.when(pair == 0)
    def _():
        row = lax.broadcasted_iota(jnp.int32, (GROUP, GROUP), 0)
        col = lax.broadcasted_iota(jnp.int32, (GROUP, GROUP), 1)
        for g in range(groups):
            at = pl.ds(g * GROUP, GROUP)
            both = nt(b_ref[at, :], c_ref[at, :])
            cross[at, :] = jnp.where(col >= row, both, 0.0)
        vt[...] = jnp.zeros_like(vt)
        dbc_ref[...] = jnp.zeros_like(dbc_ref)

    running = sin_ref[0]
    grads = []
    for g in range(groups):
        at = pl.ds(g * GROUP, GROUP)
        cols = tab_ref[0, :, at].T
        el = pair_wide(cols, EL, first)
        xw = x_ref[at, :].astype(F32) * (pair_wide(cols, DT, first) * pair_wide(cols, FE, first))
        yw = dy_ref[at, :].astype(F32) * el
        starts[g] = running
        decay = el[GROUP - 1 :, :]
        running = decay * running + tn(b_ref[at, :], xw.astype(BF16))
        grads.append((decay, tn(c_ref[at, :], yw.astype(BF16))))
    running = gin_ref[0]
    for g in range(groups - 1, -1, -1):
        ends[g] = running
        running = grads[g][0] * running + grads[g][1]

    for g in range(groups):
        at = pl.ds(g * GROUP, GROUP)
        tab = tab_ref[0, :, at]
        cols = tab.T
        el = pair_wide(cols, EL, first)
        fe = pair_wide(cols, FE, first)
        dt = pair_wide(cols, DT, first)
        x = x_ref[at, :]
        dy = dy_ref[at, :]
        xf = x.astype(F32)
        yf = dy.astype(F32)
        start = starts[g]
        end = ends[g]
        start_low = start.astype(BF16)
        end_low = end.astype(BF16)
        bg = b_ref[at, :]
        cg = c_ref[at, :]
        yw = yf * el
        xd = xf * dt
        g_end = nn(bg, end_low) * fe
        backward = yw * nn(cg, start_low)
        dbc_ref[at, :state] += nt((xd * fe).astype(BF16), end_low)
        dbc_ref[at, state:] += nt(yw.astype(BF16), start_low)
        intra = []
        for h in range(2):
            keep = first if h == 0 else jnp.logical_not(first)
            xm = jnp.where(keep, xf, 0.0).astype(BF16)
            l_row = tab[h * ROWS + L2 : h * ROWS + L2 + 1, :]
            parts = []
            col_sum = None
            weighted = None
            for a in range(GROUP // HALF):
                lo = a * HALF
                rows = slice(lo, lo + HALF)
                here = pl.ds(g * GROUP + lo, HALF)
                l_col = cols[rows, h * ROWS + L2 : h * ROWS + L2 + 1]
                dt_col = cols[rows, h * ROWS + DT : h * ROWS + DT + 1]
                q = jnp.exp2(jnp.minimum(l_row[:, lo:] - l_col, 0.0))
                cb = cross[here, lo:]
                mix = (cb * q).astype(BF16)
                parts.append(nn(mix, dy[lo:, :]))
                z = nt(xm[rows, :], dy[lo:, :]) * q * dt_col
                vt[here, lo:] += z
                box = cb * z
                down = jnp.sum(box, axis=0, keepdims=True)
                across = jnp.sum(box, axis=1, keepdims=True)
                row_w = jnp.sum(cols[rows, :] * across, axis=0, keepdims=True)
                if a == 0:
                    col_sum, weighted = down, row_w
                else:
                    col_sum = col_sum + jnp.concatenate(
                        [jnp.zeros((1, lo), F32), down], axis=1
                    )
                    weighted = weighted + row_w
            intra.append(jnp.concatenate(parts, axis=0))
            small_ref[0, g, h : h + 1, :] = col_sum
            small_ref[0, g, 2 + h : 3 + h, : 2 * ROWS] = weighted
        total = jnp.where(first, intra[0], intra[1]) + g_end
        dx_ref[at, :] = (dt * total + skip_ref[...] * yf).astype(BF16)
        products = jnp.concatenate([backward, xd * g_end, xf * total], axis=1)
        sums_ref[0, g] = nn(tab, products, HIGH)
        small_ref[0, g, 4:5, :128] = jnp.sum(start * end, axis=0, keepdims=True)
        small_ref[0, g, 5:6, :128] = jnp.sum(xf * yf, axis=0, keepdims=True)

    @pl.when(pair == pl.num_programs(0) - 1)
    def _():
        row = lax.broadcasted_iota(jnp.int32, (GROUP, GROUP), 0)
        col = lax.broadcasted_iota(jnp.int32, (GROUP, GROUP), 1)
        for g in range(groups):
            at = pl.ds(g * GROUP, GROUP)
            v = jnp.where(col >= row, vt[at, :], 0.0).astype(BF16)
            dbc_ref[at, :state] += nn(v, c_ref[at, :])
            dbc_ref[at, state:] += tn(v, b_ref[at, :])


def chain_kernel(n, s_ref, g_ref, e_ref, sin_ref, gin_ref, s_in, g_in, s_out, g_out,
                 s_send, s_recv, g_send, g_recv):
    me = lax.axis_index("seq")
    chunks = s_ref.shape[0]
    up = lax.rem(me + 1, n)
    down = lax.rem(me + n - 1, n)
    barrier = pltpu.get_barrier_semaphore()
    for other in (up, down):
        pl.semaphore_signal(barrier, inc=1, device_id={"seq": other}, device_id_type=MESH)
    pl.semaphore_wait(barrier, 2)

    def copy(c, out, into, send, recv, target):
        return pltpu.make_async_remote_copy(
            src_ref=out.at[c], dst_ref=into.at[c], send_sem=send.at[c], recv_sem=recv.at[c],
            device_id={"seq": target}, device_id_type=MESH,
        )

    def hop(c, hops, own, result, out, into, send, recv, target):
        @pl.when(hops == 0)
        def _():
            result[c] = jnp.zeros(result.shape[1:], F32)

        @pl.when(hops > 0)
        def _():
            copy(c, out, into, send, recv, target).wait_recv()
            result[c] = into[c]

        @pl.when(hops < n - 1)
        def _():
            out[c] = e_ref[c, :1, :] * result[c] + own[c]
            copy(c, out, into, send, recv, target).start()

    lag = 2

    def slot(k, carry):
        c = k - lag * me

        @pl.when(jnp.logical_and(c >= 0, c < chunks))
        def _():
            hop(c, me, s_ref, sin_ref, s_out, s_in, s_send, s_recv, up)

        far = n - 1 - me
        d = k - lag * far

        @pl.when(jnp.logical_and(d >= 0, d < chunks))
        def _():
            hop(d, far, g_ref, gin_ref, g_out, g_in, g_send, g_recv, down)

        return carry

    lax.fori_loop(0, lag * (n - 1) + chunks, slot, 0)

    @pl.when(me < n - 1)
    def _():
        for c in range(chunks):
            copy(c, s_out, s_in, s_send, s_recv, up).wait_send()

    @pl.when(me > 0)
    def _():
        for c in range(chunks):
            copy(c, g_out, g_in, g_send, g_recv, down).wait_send()


def ring_place(i, n):
    if n % 2:
        return lax.rem(i + n, n)
    return jnp.where(lax.rem(i, 2) == 0, lax.div(i, 2), n - 1 - lax.div(i, 2))


def ring_index(p, n):
    p = lax.rem(p + 2 * n, n)
    if n % 2:
        return p
    return jnp.where(p < n // 2, 2 * p, 2 * (n - 1 - p) + 1)


def ring_kernel(n, q, lt_ref, dx_ref, st_ref, out_ref, sto_ref, slots, peers,
                send, recv, st_send, st_recv):
    me = lax.axis_index("seq")
    p = ring_place(me, n)
    targets = (ring_index(p + 1, n), ring_index(p - 1, n))
    half = slots.shape[3]
    width = slots.shape[4]
    barrier = pltpu.get_barrier_semaphore()
    for j in range(1, n):
        pl.semaphore_signal(
            barrier, inc=1, device_id={"seq": lax.rem(me + j, n)}, device_id_type=MESH
        )
    pl.semaphore_wait(barrier, n - 1)

    def own(s, d, k):
        block = ring_index(p - 1 - s, n) if d == 0 else ring_index(p + 1 + s, n)
        return nn(lt_ref[2 * block + d], dx_ref[:, k * width : (k + 1) * width])

    def copy(s, d, k):
        return pltpu.make_async_remote_copy(
            src_ref=slots.at[s, d, k], dst_ref=slots.at[s + 1, d, k],
            send_sem=send.at[s, d, k], recv_sem=recv.at[s + 1, d, k],
            device_id={"seq": targets[d]}, device_id_type=MESH,
        )

    def stat(j):
        return pltpu.make_async_remote_copy(
            src_ref=st_ref, dst_ref=peers.at[j], send_sem=st_send.at[j], recv_sem=st_recv.at[j],
            device_id={"seq": lax.rem(me + j, n)}, device_id_type=MESH,
        )

    for k in range(q):
        for d in range(2):
            slots[0, d, k] = own(0, d, k)
            copy(0, d, k).start()
    for j in range(1, n):
        stat(j).start()

    def step(s, carry):
        for k in range(q):
            for d in range(2):
                mine = own(s, d, k)
                copy(s - 1, d, k).wait_recv()
                slots[s, d, k] = slots[s, d, k] + mine
                copy(s, d, k).start()
        return carry

    lax.fori_loop(1, n - 1, step, 0)
    for k in range(q):
        for d in range(2):
            mine = own(n - 1, d, k)
            copy(n - 2, d, k).wait_recv()
            out_ref[d * half : (d + 1) * half, k * width : (k + 1) * width] = (
                slots[n - 1, d, k] + mine
            )
    total = st_ref[...]
    for j in range(1, n):
        stat(j).wait_recv()
        total = total + peers[j]
    sto_ref[...] = total

    def drain(s, carry):
        for k in range(q):
            for d in range(2):
                copy(s, d, k).wait_send()
        return carry

    lax.fori_loop(0, n - 1, drain, 0)
    for j in range(1, n):
        stat(j).wait_send()


def vmem(count):
    return [pl.BlockSpec(memory_space=pltpu.VMEM)] * count


def on_device(layer_in, ssm_input, b_matrix, c_matrix, dt_raw, dt_bias, a_log, d_skip, grad_out):
    n = lax.axis_size("seq")
    tok, heads = dt_raw.shape
    width = ssm_input.shape[1]
    dim = width // heads
    state = b_matrix.shape[1]
    groups = tok // GROUP
    pairs = heads // 2
    depth = layer_in.shape[1]

    shifted = dt_raw.T + dt_bias[:, None]
    dt = jax.nn.softplus(shifted)
    slope = jax.nn.sigmoid(shifted)
    rate = -jnp.exp(a_log)
    step = dt * rate[:, None]
    stacked = jnp.stack([step, dt, slope]).reshape(3, heads, groups, GROUP)
    tri = jnp.triu(jnp.ones((GROUP, GROUP), F32))
    sums = lax.dot_general(
        stacked, tri, (((3,), (0,)), ((), ())), precision=HIGH, preferred_element_type=F32
    )
    within, up_dt, up_sl = sums[0], sums[1], sums[2]
    last = sums[..., -1:]
    lend = within[..., -1:]
    offset = jnp.cumsum(lend, axis=1) - lend
    bend = jnp.sum(lend, axis=1, keepdims=True)
    cumulative = within + offset
    after = last[1:] - sums[1:]
    fall = jnp.exp(lend - within)
    dt3 = dt.reshape(heads, groups, GROUP)
    rows = [
        within * LOG2E, dt3, jnp.exp(within), fall, slope.reshape(heads, groups, GROUP),
        up_dt, up_sl, after[0], after[1], dt3 * jnp.exp(bend - cumulative), jnp.exp(cumulative),
    ]
    rows = rows + [jnp.zeros_like(within)] * (ROWS - len(rows))
    table = jnp.stack(rows, axis=1).reshape(pairs, 2 * ROWS, tok)

    wide = pl.BlockSpec((tok, 2 * dim), lambda i: (0, i))
    whole = pl.BlockSpec((tok, state), lambda i: (0, 0))
    tab_spec = pl.BlockSpec((1, 2 * ROWS, tok), lambda i: (i, 0, 0))
    square = pl.BlockSpec((1, state, 2 * dim), lambda i: (i, 0, 0))
    states = jax.ShapeDtypeStruct((pairs, state, 2 * dim), F32)
    block_state, block_grad = pl.pallas_call(
        states_kernel,
        grid=(pairs,),
        in_specs=[wide, wide, whole, whole, tab_spec],
        out_specs=[square, square],
        out_shape=[states, states],
        name="block_states",
    )(ssm_input, grad_out, b_matrix, c_matrix, table)

    decay = jnp.repeat(jnp.exp(bend[:, 0, 0]), dim).reshape(pairs, 1, 2 * dim)
    decay = jnp.broadcast_to(decay, (pairs, 8, 2 * dim))
    buffers = pltpu.VMEM((pairs, state, 2 * dim), F32)
    sems = pltpu.SemaphoreType.DMA((pairs,))
    state_in, grad_in = pl.pallas_call(
        partial(chain_kernel, n),
        in_specs=vmem(3),
        out_specs=vmem(2),
        out_shape=[states, states],
        scratch_shapes=[buffers] * 4 + [sems] * 4,
        compiler_params=pltpu.CompilerParams(collective_id=1, has_side_effects=True),
        name="state_chain",
    )(block_state, block_grad, decay)

    skip_row = jnp.repeat(d_skip, dim).reshape(1, width)
    dx, dbc, weighted, small = pl.pallas_call(
        partial(group_kernel, groups),
        grid=(pairs,),
        in_specs=[
            wide, wide, whole, whole, tab_spec,
            pl.BlockSpec((1, 2 * dim), lambda i: (0, i)), square, square,
        ],
        out_specs=[
            wide,
            pl.BlockSpec((tok, 2 * state), lambda i: (0, 0)),
            pl.BlockSpec((1, groups, 2 * ROWS, 6 * dim), lambda i: (i, 0, 0, 0)),
            pl.BlockSpec((1, groups, 8, GROUP), lambda i: (i, 0, 0, 0)),
        ],
        out_shape=[
            jax.ShapeDtypeStruct((tok, width), BF16),
            jax.ShapeDtypeStruct((tok, 2 * state), F32),
            jax.ShapeDtypeStruct((pairs, groups, 2 * ROWS, 6 * dim), F32),
            jax.ShapeDtypeStruct((pairs, groups, 8, GROUP), F32),
        ],
        scratch_shapes=[
            pltpu.VMEM((tok, GROUP), F32),
            pltpu.VMEM((tok, GROUP), F32),
            pltpu.VMEM((groups, state, 2 * dim), F32),
            pltpu.VMEM((groups, state, 2 * dim), F32),
        ],
        name="group_terms",
    )(ssm_input, grad_out, b_matrix, c_matrix, table, skip_row, state_in, grad_in)

    owned = lax.psum_scatter(dbc, "mp", scatter_dimension=1, tiled=True).astype(BF16)
    grad_wbc = lax.psum_scatter(
        lax.dot_general(
            layer_in, owned, (((0,), (0,)), ((), ())), preferred_element_type=F32
        ),
        "seq", scatter_dimension=0, tiled=True,
    )

    folded = jnp.sum(
        weighted.reshape(pairs, groups, 2, ROWS, 3, 2, dim), axis=(1, 6)
    )
    own = jnp.stack([folded[:, 0, :, :, 0], folded[:, 1, :, :, 1]], axis=1)
    own = own.reshape(heads, ROWS, 3)
    row_w = jnp.stack(
        [small[:, :, 2, :ROWS], small[:, :, 3, ROWS : 2 * ROWS]], axis=1
    ).sum(axis=2).reshape(heads, ROWS)
    col_sum = jnp.swapaxes(small[:, :, :2, :], 1, 2).reshape(heads, groups, GROUP)
    meet = small[:, :, 4, : 2 * dim].reshape(pairs, groups, 2, dim).sum(axis=3)
    meet = jnp.swapaxes(meet, 1, 2).reshape(heads, groups) * jnp.exp(lend[..., 0])
    skip_sum = small[:, :, 5, : 2 * dim].reshape(pairs, groups, 2, dim).sum(axis=(1, 3))

    def through(ups, up_row, after_row, k):
        return (
            own[:, up_row, 0] + own[:, after_row, 1]
            + jnp.sum(ups * col_sum, axis=(1, 2)) - row_w[:, up_row]
            + jnp.sum(meet * last[k, :, :, 0], axis=1)
        )

    rate_part = through(up_dt, UPD, AFD, 1)
    bias_part = own[:, SL, 2] + rate * through(up_sl, UPS, AFS, 2)
    stat = jnp.zeros((8, 128), F32)
    stat = stat.at[:3, :heads].set(
        jnp.stack([rate_part, bias_part, skip_sum.reshape(heads)])
    )

    block = depth // n
    half = block // 2
    q = 2
    lt = layer_in.T.reshape(2 * n, half, tok)
    ring = pltpu.SemaphoreType.DMA((n, 2, q))
    each = pltpu.SemaphoreType.DMA((n,))
    grad_wx, totals = pl.pallas_call(
        partial(ring_kernel, n, q),
        in_specs=vmem(3),
        out_specs=vmem(2),
        out_shape=[
            jax.ShapeDtypeStruct((block, width), F32),
            jax.ShapeDtypeStruct((8, 128), F32),
        ],
        scratch_shapes=[
            pltpu.VMEM((n, 2, q, half, width // q), F32),
            pltpu.VMEM((n, 8, 128), F32),
            ring, ring, each, each,
        ],
        compiler_params=pltpu.CompilerParams(collective_id=2, has_side_effects=True),
        cost_estimate=pl.CostEstimate(
            flops=60 * 2 * tok * depth * width, bytes_accessed=2 * depth * width, transcendentals=0
        ),
        name="ring_projection",
    )(lt, dx, stat)
    return (
        grad_wx, grad_wbc, rate * totals[0, :heads], totals[1, :heads], totals[2, :heads],
    )


def solution(mesh):
    in_specs = (
        P("seq", None),
        P("seq", "mp"),
        P("seq", None),
        P("seq", None),
        P("seq", "mp"),
        P("mp"),
        P("mp"),
        P("mp"),
        P("seq", "mp"),
    )
    out_specs = (P("seq", "mp"), P("seq", "mp"), P("mp"), P("mp"), P("mp"))
    return jax.shard_map(
        on_device, mesh=mesh, in_specs=in_specs, out_specs=out_specs, check_vma=False
    )
```

```python
from functools import partial

import jax
import jax.numpy as jnp
from jax import lax
from jax.experimental import pallas as pl
from jax.experimental.pallas import tpu as pltpu
from jax.sharding import PartitionSpec as P

GROUP = 256
HALF = 128
ROWS = 16
LOG2E = 1.4426950408889634
HIGH = lax.Precision.HIGHEST
MESH = pl.DeviceIdType.MESH
F32 = jnp.float32
BF16 = jnp.bfloat16
L2, DT, EL, FE, SL, UPD, UPS, AFD, AFS, XB, YB = range(11)


def nn(a, b, precision=None):
    return lax.dot_general(
        a, b, (((1,), (0,)), ((), ())), precision=precision, preferred_element_type=F32
    )


def nt(a, b):
    return lax.dot_general(a, b, (((1,), (1,)), ((), ())), preferred_element_type=F32)


def tn(a, b):
    return lax.dot_general(a, b, (((0,), (0,)), ((), ())), preferred_element_type=F32)


def pair_wide(cols, row, first):
    low = cols[:, row : row + 1]
    high = cols[:, ROWS + row : ROWS + row + 1]
    return jnp.where(first, low, high)


def states_kernel(x_ref, dy_ref, b_ref, c_ref, tab_ref, s_ref, g_ref):
    cols = tab_ref[0].T
    first = lax.broadcasted_iota(jnp.int32, (1, 128), 1) < 64
    xb = (x_ref[...].astype(F32) * pair_wide(cols, XB, first)).astype(BF16)
    yb = (dy_ref[...].astype(F32) * pair_wide(cols, YB, first)).astype(BF16)
    s_ref[0] = tn(b_ref[...], xb)
    g_ref[0] = tn(c_ref[...], yb)


def group_kernel(
    groups, x_ref, dy_ref, b_ref, c_ref, tab_ref, skip_ref, sin_ref, gin_ref, layer_ref,
    dx_ref, out_ref, sums_ref, small_ref, turned_ref, cross, vt, starts, ends, dbc_ref,
):
    pair = pl.program_id(0)
    state = b_ref.shape[1]
    first = lax.broadcasted_iota(jnp.int32, (1, 128), 1) < 64

    @pl.when(pair == 0)
    def _():
        row = lax.broadcasted_iota(jnp.int32, (GROUP, GROUP), 0)
        col = lax.broadcasted_iota(jnp.int32, (GROUP, GROUP), 1)
        for g in range(groups):
            at = pl.ds(g * GROUP, GROUP)
            both = nt(b_ref[at, :], c_ref[at, :])
            cross[at, :] = jnp.where(col >= row, both, 0.0)
        vt[...] = jnp.zeros_like(vt)
        dbc_ref[...] = jnp.zeros_like(dbc_ref)

    turned_ref[...] = layer_ref[...].T
    running = sin_ref[0]
    grads = []
    for g in range(groups):
        at = pl.ds(g * GROUP, GROUP)
        cols = tab_ref[0, :, at].T
        el = pair_wide(cols, EL, first)
        xw = x_ref[at, :].astype(F32) * (pair_wide(cols, DT, first) * pair_wide(cols, FE, first))
        yw = dy_ref[at, :].astype(F32) * el
        starts[g] = running
        decay = el[GROUP - 1 :, :]
        running = decay * running + tn(b_ref[at, :], xw.astype(BF16))
        grads.append((decay, tn(c_ref[at, :], yw.astype(BF16))))
    running = gin_ref[0]
    for g in range(groups - 1, -1, -1):
        ends[g] = running
        running = grads[g][0] * running + grads[g][1]

    for g in range(groups):
        at = pl.ds(g * GROUP, GROUP)
        tab = tab_ref[0, :, at]
        cols = tab.T
        el = pair_wide(cols, EL, first)
        fe = pair_wide(cols, FE, first)
        dt = pair_wide(cols, DT, first)
        x = x_ref[at, :]
        dy = dy_ref[at, :]
        xf = x.astype(F32)
        yf = dy.astype(F32)
        start = starts[g]
        end = ends[g]
        start_low = start.astype(BF16)
        end_low = end.astype(BF16)
        bg = b_ref[at, :]
        cg = c_ref[at, :]
        yw = yf * el
        xd = xf * dt
        g_end = nn(bg, end_low) * fe
        backward = yw * nn(cg, start_low)
        dbc_ref[at, :state] += nt((xd * fe).astype(BF16), end_low)
        dbc_ref[at, state:] += nt(yw.astype(BF16), start_low)
        intra = []
        for h in range(2):
            keep = first if h == 0 else jnp.logical_not(first)
            xm = jnp.where(keep, xf, 0.0).astype(BF16)
            l_row = tab[h * ROWS + L2 : h * ROWS + L2 + 1, :]
            parts = []
            col_sum = None
            weighted = None
            for a in range(GROUP // HALF):
                lo = a * HALF
                rows = slice(lo, lo + HALF)
                here = pl.ds(g * GROUP + lo, HALF)
                l_col = cols[rows, h * ROWS + L2 : h * ROWS + L2 + 1]
                dt_col = cols[rows, h * ROWS + DT : h * ROWS + DT + 1]
                q = jnp.exp2(jnp.minimum(l_row[:, lo:] - l_col, 0.0))
                cb = cross[here, lo:]
                mix = (cb * q).astype(BF16)
                parts.append(nn(mix, dy[lo:, :]))
                z = nt(xm[rows, :], dy[lo:, :]) * q * dt_col
                vt[here, lo:] += z
                box = cb * z
                down = jnp.sum(box, axis=0, keepdims=True)
                across = jnp.sum(box, axis=1, keepdims=True)
                row_w = jnp.sum(cols[rows, :] * across, axis=0, keepdims=True)
                if a == 0:
                    col_sum, weighted = down, row_w
                else:
                    col_sum = col_sum + jnp.concatenate(
                        [jnp.zeros((1, lo), F32), down], axis=1
                    )
                    weighted = weighted + row_w
            intra.append(jnp.concatenate(parts, axis=0))
            small_ref[0, g, h : h + 1, :] = col_sum
            small_ref[0, g, 2 + h : 3 + h, : 2 * ROWS] = weighted
        total = jnp.where(first, intra[0], intra[1]) + g_end
        dx_ref[at, :] = (dt * total + skip_ref[...] * yf).astype(BF16)
        products = jnp.concatenate([backward, xd * g_end, xf * total], axis=1)
        sums_ref[0, g] = nn(tab, products, HIGH)
        small_ref[0, g, 4:5, :128] = jnp.sum(start * end, axis=0, keepdims=True)
        small_ref[0, g, 5:6, :128] = jnp.sum(xf * yf, axis=0, keepdims=True)

    @pl.when(pair == pl.num_programs(0) - 1)
    def _():
        row = lax.broadcasted_iota(jnp.int32, (GROUP, GROUP), 0)
        col = lax.broadcasted_iota(jnp.int32, (GROUP, GROUP), 1)
        for g in range(groups):
            at = pl.ds(g * GROUP, GROUP)
            v = jnp.where(col >= row, vt[at, :], 0.0).astype(BF16)
            dbc_ref[at, :state] += nn(v, c_ref[at, :])
            dbc_ref[at, state:] += tn(v, b_ref[at, :])
        out_ref[...] = dbc_ref[...].T


def chain_kernel(n, s_ref, g_ref, e_ref, sin_ref, gin_ref, mate, mate_e, passed, lent, made,
                 mate_send, mate_recv, e_sem, pass_send, pass_recv, lend_send, lend_recv):
    me = lax.axis_index("seq")
    chunks = s_ref.shape[0]
    steps = n // 2
    odd = lax.rem(me, 2)
    place = lax.div(me, 2)
    partner = me + 1 - 2 * odd
    up = lax.rem(me + 2, n)
    down = lax.rem(me + n - 2, n)
    barrier = pltpu.get_barrier_semaphore()
    for other in (partner, up, down):
        pl.semaphore_signal(barrier, inc=1, device_id={"seq": other}, device_id_type=MESH)
    pl.semaphore_wait(barrier, 3)

    def remote(src, dst, send, recv, target):
        return pltpu.make_async_remote_copy(
            src_ref=src, dst_ref=dst, send_sem=send, recv_sem=recv,
            device_id={"seq": target}, device_id_type=MESH,
        )

    def run(tail_own, tail_in, tail_hops, target, head_own, head_in):
        head_hops = steps - 1 - tail_hops

        def to_mate(c):
            return remote(head_own.at[c], mate.at[c], mate_send.at[c], mate_recv.at[c], partner)

        def onward(c):
            return remote(made.at[c], passed.at[c], pass_send.at[c], pass_recv.at[c], target)

        def aside(c):
            return remote(passed.at[c], lent.at[c], lend_send.at[c], lend_recv.at[c], partner)

        decay = remote(e_ref, mate_e, e_sem.at[0], e_sem.at[1], partner)
        decay.start()
        for c in range(chunks):
            to_mate(c).start()
        decay.wait_recv()
        lag = 2

        def slot(k, carry):
            c = k - lag * tail_hops
            d = k - lag * head_hops - 2

            @pl.when(jnp.logical_and(c >= 0, c < chunks))
            def _():
                to_mate(c).wait_recv()

                @pl.when(tail_hops == 0)
                def _():
                    tail_in[c] = mate[c]

                @pl.when(tail_hops > 0)
                def _():
                    onward(c).wait_recv()
                    aside(c).start()
                    tail_in[c] = mate_e[c, :1, :] * passed[c] + mate[c]

                @pl.when(tail_hops < steps - 1)
                def _():
                    made[c] = e_ref[c, :1, :] * tail_in[c] + tail_own[c]
                    onward(c).start()

            @pl.when(jnp.logical_and(d >= 0, d < chunks))
            def _():
                @pl.when(head_hops == 0)
                def _():
                    head_in[d] = jnp.zeros(head_in.shape[1:], F32)

                @pl.when(head_hops > 0)
                def _():
                    aside(d).wait_recv()
                    head_in[d] = lent[d]

            return carry

        lax.fori_loop(0, lag * (steps - 1) + chunks + 2, slot, 0)
        decay.wait_send()
        for c in range(chunks):
            to_mate(c).wait_send()

        @pl.when(tail_hops > 0)
        def _():
            for c in range(chunks):
                aside(c).wait_send()

        @pl.when(tail_hops < steps - 1)
        def _():
            for c in range(chunks):
                onward(c).wait_send()

    @pl.when(odd == 1)
    def _():
        run(s_ref, sin_ref, place, up, g_ref, gin_ref)

    @pl.when(odd == 0)
    def _():
        run(g_ref, gin_ref, steps - 1 - place, down, s_ref, sin_ref)


def ring_place(i, n):
    if n % 2:
        return lax.rem(i + n, n)
    return jnp.where(lax.rem(i, 2) == 0, lax.div(i, 2), n - 1 - lax.div(i, 2))


def ring_index(p, n):
    p = lax.rem(p + 2 * n, n)
    if n % 2:
        return p
    return jnp.where(p < n // 2, 2 * p, 2 * (n - 1 - p) + 1)


def ring_kernel(n, m, q, lt_ref, dx_ref, bc_ref, st_ref, out_ref, wbc_ref, sto_ref,
                slots, narrow, low, others, peers,
                send, recv, n_send, n_recv, o_send, o_recv, st_send, st_recv):
    me = lax.axis_index("seq")
    mine_mp = lax.axis_index("mp")
    p = ring_place(me, n)
    targets = (ring_index(p + 1, n), ring_index(p - 1, n))
    half = slots.shape[3]
    width = slots.shape[4]
    barrier = pltpu.get_barrier_semaphore()
    for j in range(1, n):
        pl.semaphore_signal(
            barrier, inc=1, device_id={"seq": lax.rem(me + j, n)}, device_id_type=MESH
        )
    for j in range(1, m):
        pl.semaphore_signal(
            barrier, inc=1, device_id={"mp": lax.rem(mine_mp + j, m)}, device_id_type=MESH
        )
    pl.semaphore_wait(barrier, n + m - 2)
    cols = low.shape[0]
    quarter = half // 2

    def own_narrow(s, d):
        block = ring_index(p - 1 - s, n) if d == 0 else ring_index(p + 1 + s, n)
        both = nt(lt_ref[2 * block + d], low[...])
        return jnp.concatenate([both[:quarter], both[quarter:]], axis=1)

    def copy_narrow(s, d):
        return pltpu.make_async_remote_copy(
            src_ref=narrow.at[s, d], dst_ref=narrow.at[s + 1, d],
            send_sem=n_send.at[s, d], recv_sem=n_recv.at[s + 1, d],
            device_id={"seq": targets[d]}, device_id_type=MESH,
        )

    def other(j):
        at = lax.rem(mine_mp + j, m)
        return pltpu.make_async_remote_copy(
            src_ref=bc_ref.at[at], dst_ref=others.at[j],
            send_sem=o_send.at[j], recv_sem=o_recv.at[j],
            device_id={"mp": at}, device_id_type=MESH,
        )

    for j in range(1, m):
        other(j).start()

    def own(s, d, k):
        block = ring_index(p - 1 - s, n) if d == 0 else ring_index(p + 1 + s, n)
        return nn(lt_ref[2 * block + d], dx_ref[:, k * width : (k + 1) * width])

    def copy(s, d, k):
        return pltpu.make_async_remote_copy(
            src_ref=slots.at[s, d, k], dst_ref=slots.at[s + 1, d, k],
            send_sem=send.at[s, d, k], recv_sem=recv.at[s + 1, d, k],
            device_id={"seq": targets[d]}, device_id_type=MESH,
        )

    def stat(j):
        return pltpu.make_async_remote_copy(
            src_ref=st_ref, dst_ref=peers.at[j], send_sem=st_send.at[j], recv_sem=st_recv.at[j],
            device_id={"seq": lax.rem(me + j, n)}, device_id_type=MESH,
        )

    for k in range(q):
        for d in range(2):
            slots[0, d, k] = own(0, d, k)
            copy(0, d, k).start()
    for j in range(1, n):
        stat(j).start()
    summed = bc_ref[mine_mp]
    for j in range(1, m):
        other(j).wait_recv()
        summed = summed + others[j]
    low[...] = summed.astype(BF16)
    for d in range(2):
        narrow[0, d] = own_narrow(0, d)
        copy_narrow(0, d).start()

    def step(s, carry):
        for k in range(q):
            for d in range(2):
                mine = own(s, d, k)
                copy(s - 1, d, k).wait_recv()
                slots[s, d, k] = slots[s, d, k] + mine
                copy(s, d, k).start()
        for d in range(2):
            mine = own_narrow(s, d)
            copy_narrow(s - 1, d).wait_recv()
            narrow[s, d] = narrow[s, d] + mine
            copy_narrow(s, d).start()
        return carry

    lax.fori_loop(1, n - 1, step, 0)
    for k in range(q):
        for d in range(2):
            mine = own(n - 1, d, k)
            copy(n - 2, d, k).wait_recv()
            out_ref[d * half : (d + 1) * half, k * width : (k + 1) * width] = (
                slots[n - 1, d, k] + mine
            )
    for d in range(2):
        mine = own_narrow(n - 1, d)
        copy_narrow(n - 2, d).wait_recv()
        both = narrow[n - 1, d] + mine
        wbc_ref[d * half : d * half + quarter, :] = both[:, :cols]
        wbc_ref[d * half + quarter : (d + 1) * half, :] = both[:, cols:]
    total = st_ref[...]
    for j in range(1, n):
        stat(j).wait_recv()
        total = total + peers[j]
    sto_ref[...] = total

    def drain(s, carry):
        for k in range(q):
            for d in range(2):
                copy(s, d, k).wait_send()
        for d in range(2):
            copy_narrow(s, d).wait_send()
        return carry

    lax.fori_loop(0, n - 1, drain, 0)
    for j in range(1, n):
        stat(j).wait_send()
    for j in range(1, m):
        other(j).wait_send()


def vmem(count):
    return [pl.BlockSpec(memory_space=pltpu.VMEM)] * count


def on_device(layer_in, ssm_input, b_matrix, c_matrix, dt_raw, dt_bias, a_log, d_skip, grad_out):
    n = lax.axis_size("seq")
    tok, heads = dt_raw.shape
    width = ssm_input.shape[1]
    dim = width // heads
    state = b_matrix.shape[1]
    groups = tok // GROUP
    pairs = heads // 2
    depth = layer_in.shape[1]

    shifted = dt_raw.T + dt_bias[:, None]
    dt = jax.nn.softplus(shifted)
    slope = jax.nn.sigmoid(shifted)
    rate = -jnp.exp(a_log)
    step = dt * rate[:, None]
    stacked = jnp.stack([step, dt, slope]).reshape(3, heads, groups, GROUP)
    tri = jnp.triu(jnp.ones((GROUP, GROUP), F32))
    sums = lax.dot_general(
        stacked, tri, (((3,), (0,)), ((), ())), precision=HIGH, preferred_element_type=F32
    )
    within, up_dt, up_sl = sums[0], sums[1], sums[2]
    last = sums[..., -1:]
    lend = within[..., -1:]
    offset = jnp.cumsum(lend, axis=1) - lend
    bend = jnp.sum(lend, axis=1, keepdims=True)
    later = jnp.exp(jnp.minimum(bend - offset - lend, 0.0))
    cumulative = within + offset
    after = last[1:] - sums[1:]
    fall = jnp.exp(lend - within)
    dt3 = dt.reshape(heads, groups, GROUP)
    rows = [
        within * LOG2E, dt3, jnp.exp(within), fall, slope.reshape(heads, groups, GROUP),
        up_dt, up_sl, after[0], after[1], dt3 * fall * later, jnp.exp(cumulative),
    ]
    rows = rows + [jnp.zeros_like(within)] * (ROWS - len(rows))
    table = jnp.stack(rows, axis=1).reshape(pairs, 2 * ROWS, tok)

    wide = pl.BlockSpec((tok, 2 * dim), lambda i: (0, i))
    whole = pl.BlockSpec((tok, state), lambda i: (0, 0))
    tab_spec = pl.BlockSpec((1, 2 * ROWS, tok), lambda i: (i, 0, 0))
    square = pl.BlockSpec((1, state, 2 * dim), lambda i: (i, 0, 0))
    states = jax.ShapeDtypeStruct((pairs, state, 2 * dim), F32)
    block_state, block_grad = pl.pallas_call(
        states_kernel,
        grid=(pairs,),
        in_specs=[wide, wide, whole, whole, tab_spec],
        out_specs=[square, square],
        out_shape=[states, states],
        name="block_states",
    )(ssm_input, grad_out, b_matrix, c_matrix, table)

    decay = jnp.repeat(jnp.exp(bend[:, 0, 0]), dim).reshape(pairs, 1, 2 * dim)
    decay = jnp.broadcast_to(decay, (pairs, 8, 2 * dim))
    buffers = pltpu.VMEM((pairs, state, 2 * dim), F32)
    sems = pltpu.SemaphoreType.DMA((pairs,))
    state_in, grad_in = pl.pallas_call(
        partial(chain_kernel, n),
        in_specs=vmem(3),
        out_specs=vmem(2),
        out_shape=[states, states],
        scratch_shapes=[
            buffers, pltpu.VMEM((pairs, 8, 2 * dim), F32), buffers, buffers, buffers,
            sems, sems, pltpu.SemaphoreType.DMA((2,)), sems, sems, sems, sems,
        ],
        compiler_params=pltpu.CompilerParams(collective_id=1, has_side_effects=True),
        name="state_chain",
    )(block_state, block_grad, decay)

    skip_row = jnp.repeat(d_skip, dim).reshape(1, width)
    share = depth // pairs
    dx, dbc, weighted, small, turned = pl.pallas_call(
        partial(group_kernel, groups),
        grid=(pairs,),
        in_specs=[
            wide, wide, whole, whole, tab_spec,
            pl.BlockSpec((1, 2 * dim), lambda i: (0, i)), square, square,
            pl.BlockSpec((tok, share), lambda i: (0, i)),
        ],
        out_specs=[
            wide,
            pl.BlockSpec((2 * state, tok), lambda i: (0, 0)),
            pl.BlockSpec((1, groups, 2 * ROWS, 6 * dim), lambda i: (i, 0, 0, 0)),
            pl.BlockSpec((1, groups, 8, GROUP), lambda i: (i, 0, 0, 0)),
            pl.BlockSpec((share, tok), lambda i: (i, 0)),
        ],
        out_shape=[
            jax.ShapeDtypeStruct((tok, width), BF16),
            jax.ShapeDtypeStruct((2 * state, tok), F32),
            jax.ShapeDtypeStruct((pairs, groups, 2 * ROWS, 6 * dim), F32),
            jax.ShapeDtypeStruct((pairs, groups, 8, GROUP), F32),
            jax.ShapeDtypeStruct((depth, tok), BF16),
        ],
        scratch_shapes=[
            pltpu.VMEM((tok, GROUP), F32),
            pltpu.VMEM((tok, GROUP), F32),
            pltpu.VMEM((groups, state, 2 * dim), F32),
            pltpu.VMEM((groups, state, 2 * dim), F32),
            pltpu.VMEM((tok, 2 * state), F32),
        ],
        name="group_terms",
    )(ssm_input, grad_out, b_matrix, c_matrix, table, skip_row, state_in, grad_in, layer_in)

    folded = jnp.sum(
        weighted.reshape(pairs, groups, 2, ROWS, 3, 2, dim), axis=(1, 6)
    )
    own = jnp.stack([folded[:, 0, :, :, 0], folded[:, 1, :, :, 1]], axis=1)
    own = own.reshape(heads, ROWS, 3)
    row_w = jnp.stack(
        [small[:, :, 2, :ROWS], small[:, :, 3, ROWS : 2 * ROWS]], axis=1
    ).sum(axis=2).reshape(heads, ROWS)
    col_sum = jnp.swapaxes(small[:, :, :2, :], 1, 2).reshape(heads, groups, GROUP)
    meet = small[:, :, 4, : 2 * dim].reshape(pairs, groups, 2, dim).sum(axis=3)
    meet = jnp.swapaxes(meet, 1, 2).reshape(heads, groups) * jnp.exp(lend[..., 0])
    skip_sum = small[:, :, 5, : 2 * dim].reshape(pairs, groups, 2, dim).sum(axis=(1, 3))

    def through(ups, up_row, after_row, k):
        return (
            own[:, up_row, 0] + own[:, after_row, 1]
            + jnp.sum(ups * col_sum, axis=(1, 2)) - row_w[:, up_row]
            + jnp.sum(meet * last[k, :, :, 0], axis=1)
        )

    rate_part = through(up_dt, UPD, AFD, 1)
    bias_part = own[:, SL, 2] + rate * through(up_sl, UPS, AFS, 2)
    stat = jnp.zeros((8, 128), F32)
    stat = stat.at[:3, :heads].set(
        jnp.stack([rate_part, bias_part, skip_sum.reshape(heads)])
    )

    block = depth // n
    half = block // 2
    q = 2
    m = lax.axis_size("mp")
    cols = 2 * state // m
    lt = turned.reshape(2 * n, half, tok)
    around = pltpu.SemaphoreType.DMA((n, 2))
    beside = pltpu.SemaphoreType.DMA((m,))
    ring = pltpu.SemaphoreType.DMA((n, 2, q))
    each = pltpu.SemaphoreType.DMA((n,))
    grad_wx, grad_wbc, totals = pl.pallas_call(
        partial(ring_kernel, n, m, q),
        in_specs=vmem(4),
        out_specs=vmem(3),
        out_shape=[
            jax.ShapeDtypeStruct((block, width), F32),
            jax.ShapeDtypeStruct((block, cols), F32),
            jax.ShapeDtypeStruct((8, 128), F32),
        ],
        scratch_shapes=[
            pltpu.VMEM((n, 2, q, half, width // q), F32),
            pltpu.VMEM((n, 2, half // 2, 2 * cols), F32),
            pltpu.VMEM((cols, tok), BF16),
            pltpu.VMEM((m, cols, tok), F32),
            pltpu.VMEM((n, 8, 128), F32),
            ring, ring, around, around, beside, beside, each, each,
        ],
        compiler_params=pltpu.CompilerParams(collective_id=2, has_side_effects=True),
        cost_estimate=pl.CostEstimate(
            flops=60 * 2 * tok * depth * width, bytes_accessed=2 * depth * width, transcendentals=0
        ),
        name="ring_projection",
    )(lt, dx, dbc.reshape(m, cols, tok), stat)
    return (
        grad_wx, grad_wbc, rate * totals[0, :heads], totals[1, :heads], totals[2, :heads],
    )


def solution(mesh):
    in_specs = (
        P("seq", None),
        P("seq", "mp"),
        P("seq", None),
        P("seq", None),
        P("seq", "mp"),
        P("mp"),
        P("mp"),
        P("mp"),
        P("seq", "mp"),
    )
    out_specs = (P("seq", "mp"), P("seq", "mp"), P("mp"), P("mp"), P("mp"))
    return jax.shard_map(
        on_device, mesh=mesh, in_specs=in_specs, out_specs=out_specs, check_vma=False
    )
```

```python
from functools import partial

import jax
import jax.numpy as jnp
from jax import lax
from jax.experimental import pallas as pl
from jax.experimental.pallas import tpu as pltpu
from jax.sharding import PartitionSpec as P

GROUP = 256
HALF = 128
ROWS = 16
LOG2E = 1.4426950408889634
HIGH = lax.Precision.HIGHEST
MESH = pl.DeviceIdType.MESH
F32 = jnp.float32
BF16 = jnp.bfloat16
L2, DT, EL, FE, SL, UPD, UPS, AFD, AFS, XB, YB = range(11)


def nn(a, b, precision=None):
    return lax.dot_general(
        a, b, (((1,), (0,)), ((), ())), precision=precision, preferred_element_type=F32
    )


def nt(a, b):
    return lax.dot_general(a, b, (((1,), (1,)), ((), ())), preferred_element_type=F32)


def tn(a, b):
    return lax.dot_general(a, b, (((0,), (0,)), ((), ())), preferred_element_type=F32)


def pair_wide(cols, row, first):
    low = cols[:, row : row + 1]
    high = cols[:, ROWS + row : ROWS + row + 1]
    return jnp.where(first, low, high)


def states_kernel(x_ref, dy_ref, b_ref, c_ref, tab_ref, s_ref, g_ref):
    cols = tab_ref[0].T
    first = lax.broadcasted_iota(jnp.int32, (1, 128), 1) < 64
    xb = (x_ref[...].astype(F32) * pair_wide(cols, XB, first)).astype(BF16)
    yb = (dy_ref[...].astype(F32) * pair_wide(cols, YB, first)).astype(BF16)
    s_ref[0] = tn(b_ref[...], xb)
    g_ref[0] = tn(c_ref[...], yb)


def group_kernel(
    groups, x_ref, dy_ref, b_ref, c_ref, tab_ref, skip_ref, sin_ref, gin_ref, layer_ref,
    dx_ref, out_ref, sums_ref, small_ref, turned_ref, cross, vt, starts, ends, dbc_ref,
):
    pair = pl.program_id(0)
    state = b_ref.shape[1]
    first = lax.broadcasted_iota(jnp.int32, (1, 128), 1) < 64

    @pl.when(pair == 0)
    def _():
        row = lax.broadcasted_iota(jnp.int32, (GROUP, GROUP), 0)
        col = lax.broadcasted_iota(jnp.int32, (GROUP, GROUP), 1)
        for g in range(groups):
            at = pl.ds(g * GROUP, GROUP)
            both = nt(b_ref[at, :], c_ref[at, :])
            cross[at, :] = jnp.where(col >= row, both, 0.0)
        vt[...] = jnp.zeros_like(vt)
        dbc_ref[...] = jnp.zeros_like(dbc_ref)

    turned_ref[...] = layer_ref[...].T
    running = sin_ref[0]
    grads = []
    for g in range(groups):
        at = pl.ds(g * GROUP, GROUP)
        cols = tab_ref[0, :, at].T
        el = pair_wide(cols, EL, first)
        xw = x_ref[at, :].astype(F32) * (pair_wide(cols, DT, first) * pair_wide(cols, FE, first))
        yw = dy_ref[at, :].astype(F32) * el
        starts[g] = running
        decay = el[GROUP - 1 :, :]
        running = decay * running + tn(b_ref[at, :], xw.astype(BF16))
        grads.append((decay, tn(c_ref[at, :], yw.astype(BF16))))
    running = gin_ref[0]
    for g in range(groups - 1, -1, -1):
        ends[g] = running
        running = grads[g][0] * running + grads[g][1]

    for g in range(groups):
        at = pl.ds(g * GROUP, GROUP)
        tab = tab_ref[0, :, at]
        cols = tab.T
        el = pair_wide(cols, EL, first)
        fe = pair_wide(cols, FE, first)
        dt = pair_wide(cols, DT, first)
        x = x_ref[at, :]
        dy = dy_ref[at, :]
        xf = x.astype(F32)
        yf = dy.astype(F32)
        start = starts[g]
        end = ends[g]
        start_low = start.astype(BF16)
        end_low = end.astype(BF16)
        bg = b_ref[at, :]
        cg = c_ref[at, :]
        yw = yf * el
        xd = xf * dt
        g_end = nn(bg, end_low) * fe
        backward = yw * nn(cg, start_low)
        dbc_ref[at, :state] += nt((xd * fe).astype(BF16), end_low)
        dbc_ref[at, state:] += nt(yw.astype(BF16), start_low)
        intra = []
        for h in range(2):
            keep = first if h == 0 else jnp.logical_not(first)
            xm = jnp.where(keep, xf, 0.0).astype(BF16)
            l_row = tab[h * ROWS + L2 : h * ROWS + L2 + 1, :]
            parts = []
            col_sum = None
            weighted = None
            for a in range(GROUP // HALF):
                lo = a * HALF
                rows = slice(lo, lo + HALF)
                here = pl.ds(g * GROUP + lo, HALF)
                l_col = cols[rows, h * ROWS + L2 : h * ROWS + L2 + 1]
                dt_col = cols[rows, h * ROWS + DT : h * ROWS + DT + 1]
                q = jnp.exp2(jnp.minimum(l_row[:, lo:] - l_col, 0.0))
                cb = cross[here, lo:]
                mix = (cb * q).astype(BF16)
                parts.append(nn(mix, dy[lo:, :]))
                z = nt(xm[rows, :], dy[lo:, :]) * q * dt_col
                vt[here, lo:] += z
                box = cb * z
                down = jnp.sum(box, axis=0, keepdims=True)
                across = jnp.sum(box, axis=1, keepdims=True)
                row_w = jnp.sum(cols[rows, :] * across, axis=0, keepdims=True)
                if a == 0:
                    col_sum, weighted = down, row_w
                else:
                    col_sum = col_sum + jnp.concatenate(
                        [jnp.zeros((1, lo), F32), down], axis=1
                    )
                    weighted = weighted + row_w
            intra.append(jnp.concatenate(parts, axis=0))
            small_ref[0, g, h : h + 1, :] = col_sum
            small_ref[0, g, 2 + h : 3 + h, : 2 * ROWS] = weighted
        total = jnp.where(first, intra[0], intra[1]) + g_end
        dx_ref[at, :] = (dt * total + skip_ref[...] * yf).astype(BF16)
        products = jnp.concatenate([backward, xd * g_end, xf * total], axis=1)
        here_sums = nn(tab, products, HIGH)
        all_sums = here_sums if g == 0 else all_sums + here_sums
        small_ref[0, g, 4:5, :128] = jnp.sum(start * end, axis=0, keepdims=True)
        small_ref[0, g, 5:6, :128] = jnp.sum(xf * yf, axis=0, keepdims=True)

    lane = lax.broadcasted_iota(jnp.int32, (products.shape[1], 128), 0)
    slot = lax.broadcasted_iota(jnp.int32, (products.shape[1], 128), 1)
    fold = jnp.where(lax.div(lane, 64) == slot, 1.0, 0.0)
    sums_ref[0] = nn(all_sums, fold, HIGH)

    @pl.when(pair == pl.num_programs(0) - 1)
    def _():
        row = lax.broadcasted_iota(jnp.int32, (GROUP, GROUP), 0)
        col = lax.broadcasted_iota(jnp.int32, (GROUP, GROUP), 1)
        for g in range(groups):
            at = pl.ds(g * GROUP, GROUP)
            v = jnp.where(col >= row, vt[at, :], 0.0).astype(BF16)
            dbc_ref[at, :state] += nn(v, c_ref[at, :])
            dbc_ref[at, state:] += tn(v, b_ref[at, :])
        out_ref[...] = dbc_ref[...].T


def chain_kernel(n, s_ref, g_ref, e_ref, sin_ref, gin_ref, mate, mate_e, passed, lent, made,
                 mate_send, mate_recv, e_sem, pass_send, pass_recv, lend_send, lend_recv):
    me = lax.axis_index("seq")
    chunks = s_ref.shape[0]
    steps = n // 2
    odd = lax.rem(me, 2)
    place = lax.div(me, 2)
    partner = me + 1 - 2 * odd
    up = lax.rem(me + 2, n)
    down = lax.rem(me + n - 2, n)
    barrier = pltpu.get_barrier_semaphore()
    for other in (partner, up, down):
        pl.semaphore_signal(barrier, inc=1, device_id={"seq": other}, device_id_type=MESH)
    pl.semaphore_wait(barrier, 3)

    def remote(src, dst, send, recv, target):
        return pltpu.make_async_remote_copy(
            src_ref=src, dst_ref=dst, send_sem=send, recv_sem=recv,
            device_id={"seq": target}, device_id_type=MESH,
        )

    def run(tail_own, tail_in, tail_hops, target, head_own, head_in):
        head_hops = steps - 1 - tail_hops

        def to_mate(c):
            return remote(head_own.at[c], mate.at[c], mate_send.at[c], mate_recv.at[c], partner)

        def onward(c):
            return remote(made.at[c], passed.at[c], pass_send.at[c], pass_recv.at[c], target)

        def aside(c):
            return remote(passed.at[c], lent.at[c], lend_send.at[c], lend_recv.at[c], partner)

        decay = remote(e_ref, mate_e, e_sem.at[0], e_sem.at[1], partner)
        decay.start()
        for c in range(chunks):
            to_mate(c).start()
        decay.wait_recv()
        lag = 2

        def slot(k, carry):
            c = k - lag * tail_hops
            d = k - lag * head_hops - 2

            @pl.when(jnp.logical_and(c >= 0, c < chunks))
            def _():
                to_mate(c).wait_recv()

                @pl.when(tail_hops == 0)
                def _():
                    tail_in[c] = mate[c]

                @pl.when(tail_hops > 0)
                def _():
                    onward(c).wait_recv()
                    aside(c).start()
                    tail_in[c] = mate_e[c, :1, :] * passed[c] + mate[c]

                @pl.when(tail_hops < steps - 1)
                def _():
                    made[c] = e_ref[c, :1, :] * tail_in[c] + tail_own[c]
                    onward(c).start()

            @pl.when(jnp.logical_and(d >= 0, d < chunks))
            def _():
                @pl.when(head_hops == 0)
                def _():
                    head_in[d] = jnp.zeros(head_in.shape[1:], F32)

                @pl.when(head_hops > 0)
                def _():
                    aside(d).wait_recv()
                    head_in[d] = lent[d]

            return carry

        lax.fori_loop(0, lag * (steps - 1) + chunks + 2, slot, 0)
        decay.wait_send()
        for c in range(chunks):
            to_mate(c).wait_send()

        @pl.when(tail_hops > 0)
        def _():
            for c in range(chunks):
                aside(c).wait_send()

        @pl.when(tail_hops < steps - 1)
        def _():
            for c in range(chunks):
                onward(c).wait_send()

    @pl.when(odd == 1)
    def _():
        run(s_ref, sin_ref, place, up, g_ref, gin_ref)

    @pl.when(odd == 0)
    def _():
        run(g_ref, gin_ref, steps - 1 - place, down, s_ref, sin_ref)


def ring_place(i, n):
    if n % 2:
        return lax.rem(i + n, n)
    return jnp.where(lax.rem(i, 2) == 0, lax.div(i, 2), n - 1 - lax.div(i, 2))


def ring_index(p, n):
    p = lax.rem(p + 2 * n, n)
    if n % 2:
        return p
    return jnp.where(p < n // 2, 2 * p, 2 * (n - 1 - p) + 1)


def ring_kernel(n, m, q, lt_ref, dx_ref, bc_ref, st_ref, out_ref, wbc_ref, sto_ref,
                slots, narrow, low, others, peers,
                send, recv, n_send, n_recv, o_send, o_recv, st_send, st_recv):
    me = lax.axis_index("seq")
    mine_mp = lax.axis_index("mp")
    p = ring_place(me, n)
    targets = (ring_index(p + 1, n), ring_index(p - 1, n))
    half = slots.shape[3]
    width = slots.shape[4]
    barrier = pltpu.get_barrier_semaphore()
    for j in range(1, n):
        pl.semaphore_signal(
            barrier, inc=1, device_id={"seq": lax.rem(me + j, n)}, device_id_type=MESH
        )
    for j in range(1, m):
        pl.semaphore_signal(
            barrier, inc=1, device_id={"mp": lax.rem(mine_mp + j, m)}, device_id_type=MESH
        )
    pl.semaphore_wait(barrier, n + m - 2)
    cols = low.shape[0]
    quarter = half // 2

    def own_narrow(s, d):
        block = ring_index(p - 1 - s, n) if d == 0 else ring_index(p + 1 + s, n)
        both = nt(lt_ref[2 * block + d], low[...])
        return jnp.concatenate([both[:quarter], both[quarter:]], axis=1)

    def copy_narrow(s, d):
        return pltpu.make_async_remote_copy(
            src_ref=narrow.at[s, d], dst_ref=narrow.at[s + 1, d],
            send_sem=n_send.at[s, d], recv_sem=n_recv.at[s + 1, d],
            device_id={"seq": targets[d]}, device_id_type=MESH,
        )

    def other(j):
        at = lax.rem(mine_mp + j, m)
        return pltpu.make_async_remote_copy(
            src_ref=bc_ref.at[at], dst_ref=others.at[j],
            send_sem=o_send.at[j], recv_sem=o_recv.at[j],
            device_id={"mp": at}, device_id_type=MESH,
        )

    for j in range(1, m):
        other(j).start()

    def own(s, d, k):
        block = ring_index(p - 1 - s, n) if d == 0 else ring_index(p + 1 + s, n)
        return nn(lt_ref[2 * block + d], dx_ref[:, k * width : (k + 1) * width])

    def copy(s, d, k):
        return pltpu.make_async_remote_copy(
            src_ref=slots.at[s, d, k], dst_ref=slots.at[s + 1, d, k],
            send_sem=send.at[s, d, k], recv_sem=recv.at[s + 1, d, k],
            device_id={"seq": targets[d]}, device_id_type=MESH,
        )

    def stat(j):
        return pltpu.make_async_remote_copy(
            src_ref=st_ref, dst_ref=peers.at[j], send_sem=st_send.at[j], recv_sem=st_recv.at[j],
            device_id={"seq": lax.rem(me + j, n)}, device_id_type=MESH,
        )

    for k in range(q):
        for d in range(2):
            slots[0, d, k] = own(0, d, k)
            copy(0, d, k).start()
    for j in range(1, n):
        stat(j).start()
    summed = bc_ref[mine_mp]
    for j in range(1, m):
        other(j).wait_recv()
        summed = summed + others[j]
    low[...] = summed.astype(BF16)
    for d in range(2):
        narrow[0, d] = own_narrow(0, d)
        copy_narrow(0, d).start()

    def step(s, carry):
        for k in range(q):
            for d in range(2):
                mine = own(s, d, k)
                copy(s - 1, d, k).wait_recv()
                slots[s, d, k] = slots[s, d, k] + mine
                copy(s, d, k).start()
        for d in range(2):
            mine = own_narrow(s, d)
            copy_narrow(s - 1, d).wait_recv()
            narrow[s, d] = narrow[s, d] + mine
            copy_narrow(s, d).start()
        return carry

    lax.fori_loop(1, n - 1, step, 0)
    for k in range(q):
        for d in range(2):
            mine = own(n - 1, d, k)
            copy(n - 2, d, k).wait_recv()
            out_ref[d * half : (d + 1) * half, k * width : (k + 1) * width] = (
                slots[n - 1, d, k] + mine
            )
    for d in range(2):
        mine = own_narrow(n - 1, d)
        copy_narrow(n - 2, d).wait_recv()
        both = narrow[n - 1, d] + mine
        wbc_ref[d * half : d * half + quarter, :] = both[:, :cols]
        wbc_ref[d * half + quarter : (d + 1) * half, :] = both[:, cols:]
    total = st_ref[...]
    for j in range(1, n):
        stat(j).wait_recv()
        total = total + peers[j]
    sto_ref[...] = total

    def drain(s, carry):
        for k in range(q):
            for d in range(2):
                copy(s, d, k).wait_send()
        for d in range(2):
            copy_narrow(s, d).wait_send()
        return carry

    lax.fori_loop(0, n - 1, drain, 0)
    for j in range(1, n):
        stat(j).wait_send()
    for j in range(1, m):
        other(j).wait_send()


def vmem(count):
    return [pl.BlockSpec(memory_space=pltpu.VMEM)] * count


def on_device(layer_in, ssm_input, b_matrix, c_matrix, dt_raw, dt_bias, a_log, d_skip, grad_out):
    n = lax.axis_size("seq")
    tok, heads = dt_raw.shape
    width = ssm_input.shape[1]
    dim = width // heads
    state = b_matrix.shape[1]
    groups = tok // GROUP
    pairs = heads // 2
    depth = layer_in.shape[1]

    shifted = dt_raw.T + dt_bias[:, None]
    dt = jax.nn.softplus(shifted)
    slope = jax.nn.sigmoid(shifted)
    rate = -jnp.exp(a_log)
    step = dt * rate[:, None]
    stacked = jnp.stack([step, dt, slope]).reshape(3, heads, groups, GROUP)
    tri = jnp.triu(jnp.ones((GROUP, GROUP), F32))
    sums = lax.dot_general(
        stacked, tri, (((3,), (0,)), ((), ())), precision=HIGH, preferred_element_type=F32
    )
    within, up_dt, up_sl = sums[0], sums[1], sums[2]
    last = sums[..., -1:]
    lend = within[..., -1:]
    offset = jnp.cumsum(lend, axis=1) - lend
    bend = jnp.sum(lend, axis=1, keepdims=True)
    later = jnp.exp(jnp.minimum(bend - offset - lend, 0.0))
    cumulative = within + offset
    after = last[1:] - sums[1:]
    fall = jnp.exp(lend - within)
    dt3 = dt.reshape(heads, groups, GROUP)
    rows = [
        within * LOG2E, dt3, jnp.exp(within), fall, slope.reshape(heads, groups, GROUP),
        up_dt, up_sl, after[0], after[1], dt3 * fall * later, jnp.exp(cumulative),
    ]
    rows = rows + [jnp.zeros_like(within)] * (ROWS - len(rows))
    table = jnp.stack(rows, axis=1).reshape(pairs, 2 * ROWS, tok)

    wide = pl.BlockSpec((tok, 2 * dim), lambda i: (0, i))
    whole = pl.BlockSpec((tok, state), lambda i: (0, 0))
    tab_spec = pl.BlockSpec((1, 2 * ROWS, tok), lambda i: (i, 0, 0))
    square = pl.BlockSpec((1, state, 2 * dim), lambda i: (i, 0, 0))
    states = jax.ShapeDtypeStruct((pairs, state, 2 * dim), F32)
    block_state, block_grad = pl.pallas_call(
        states_kernel,
        grid=(pairs,),
        in_specs=[wide, wide, whole, whole, tab_spec],
        out_specs=[square, square],
        out_shape=[states, states],
        name="block_states",
    )(ssm_input, grad_out, b_matrix, c_matrix, table)

    decay = jnp.repeat(jnp.exp(bend[:, 0, 0]), dim).reshape(pairs, 1, 2 * dim)
    decay = jnp.broadcast_to(decay, (pairs, 8, 2 * dim))
    buffers = pltpu.VMEM((pairs, state, 2 * dim), F32)
    sems = pltpu.SemaphoreType.DMA((pairs,))
    state_in, grad_in = pl.pallas_call(
        partial(chain_kernel, n),
        in_specs=vmem(3),
        out_specs=vmem(2),
        out_shape=[states, states],
        scratch_shapes=[
            buffers, pltpu.VMEM((pairs, 8, 2 * dim), F32), buffers, buffers, buffers,
            sems, sems, pltpu.SemaphoreType.DMA((2,)), sems, sems, sems, sems,
        ],
        compiler_params=pltpu.CompilerParams(collective_id=1, has_side_effects=True),
        name="state_chain",
    )(block_state, block_grad, decay)

    skip_row = jnp.repeat(d_skip, dim).reshape(1, width)
    share = depth // pairs
    dx, dbc, weighted, small, turned = pl.pallas_call(
        partial(group_kernel, groups),
        grid=(pairs,),
        in_specs=[
            wide, wide, whole, whole, tab_spec,
            pl.BlockSpec((1, 2 * dim), lambda i: (0, i)), square, square,
            pl.BlockSpec((tok, share), lambda i: (0, i)),
        ],
        out_specs=[
            wide,
            pl.BlockSpec((2 * state, tok), lambda i: (0, 0)),
            pl.BlockSpec((1, 2 * ROWS, 128), lambda i: (i, 0, 0)),
            pl.BlockSpec((1, groups, 8, GROUP), lambda i: (i, 0, 0, 0)),
            pl.BlockSpec((share, tok), lambda i: (i, 0)),
        ],
        out_shape=[
            jax.ShapeDtypeStruct((tok, width), BF16),
            jax.ShapeDtypeStruct((2 * state, tok), F32),
            jax.ShapeDtypeStruct((pairs, 2 * ROWS, 128), F32),
            jax.ShapeDtypeStruct((pairs, groups, 8, GROUP), F32),
            jax.ShapeDtypeStruct((depth, tok), BF16),
        ],
        scratch_shapes=[
            pltpu.VMEM((tok, GROUP), F32),
            pltpu.VMEM((tok, GROUP), F32),
            pltpu.VMEM((groups, state, 2 * dim), F32),
            pltpu.VMEM((groups, state, 2 * dim), F32),
            pltpu.VMEM((tok, 2 * state), F32),
        ],
        name="group_terms",
    )(ssm_input, grad_out, b_matrix, c_matrix, table, skip_row, state_in, grad_in, layer_in)

    folded = weighted[:, :, :6].reshape(pairs, 2, ROWS, 3, 2)
    own = jnp.stack([folded[:, 0, :, :, 0], folded[:, 1, :, :, 1]], axis=1)
    own = own.reshape(heads, ROWS, 3)
    row_w = jnp.stack(
        [small[:, :, 2, :ROWS], small[:, :, 3, ROWS : 2 * ROWS]], axis=1
    ).sum(axis=2).reshape(heads, ROWS)
    col_sum = jnp.swapaxes(small[:, :, :2, :], 1, 2).reshape(heads, groups, GROUP)
    meet = small[:, :, 4, : 2 * dim].reshape(pairs, groups, 2, dim).sum(axis=3)
    meet = jnp.swapaxes(meet, 1, 2).reshape(heads, groups) * jnp.exp(lend[..., 0])
    skip_sum = small[:, :, 5, : 2 * dim].reshape(pairs, groups, 2, dim).sum(axis=(1, 3))

    def through(ups, up_row, after_row, k):
        return (
            own[:, up_row, 0] + own[:, after_row, 1]
            + jnp.sum(ups * col_sum, axis=(1, 2)) - row_w[:, up_row]
            + jnp.sum(meet * last[k, :, :, 0], axis=1)
        )

    rate_part = through(up_dt, UPD, AFD, 1)
    bias_part = own[:, SL, 2] + rate * through(up_sl, UPS, AFS, 2)
    stat = jnp.zeros((8, 128), F32)
    stat = stat.at[:3, :heads].set(
        jnp.stack([rate_part, bias_part, skip_sum.reshape(heads)])
    )

    block = depth // n
    half = block // 2
    q = 5
    m = lax.axis_size("mp")
    cols = 2 * state // m
    lt = turned.reshape(2 * n, half, tok)
    around = pltpu.SemaphoreType.DMA((n, 2))
    beside = pltpu.SemaphoreType.DMA((m,))
    ring = pltpu.SemaphoreType.DMA((n, 2, q))
    each = pltpu.SemaphoreType.DMA((n,))
    grad_wx, grad_wbc, totals = pl.pallas_call(
        partial(ring_kernel, n, m, q),
        in_specs=vmem(4),
        out_specs=vmem(3),
        out_shape=[
            jax.ShapeDtypeStruct((block, width), F32),
            jax.ShapeDtypeStruct((block, cols), F32),
            jax.ShapeDtypeStruct((8, 128), F32),
        ],
        scratch_shapes=[
            pltpu.VMEM((n, 2, q, half, width // q), F32),
            pltpu.VMEM((n, 2, half // 2, 2 * cols), F32),
            pltpu.VMEM((cols, tok), BF16),
            pltpu.VMEM((m, cols, tok), F32),
            pltpu.VMEM((n, 8, 128), F32),
            ring, ring, around, around, beside, beside, each, each,
        ],
        compiler_params=pltpu.CompilerParams(collective_id=2, has_side_effects=True),
        cost_estimate=pl.CostEstimate(
            flops=60 * 2 * tok * depth * width, bytes_accessed=2 * depth * width, transcendentals=0
        ),
        name="ring_projection",
    )(lt, dx, dbc.reshape(m, cols, tok), stat)
    return (
        grad_wx, grad_wbc, rate * totals[0, :heads], totals[1, :heads], totals[2, :heads],
    )


def solution(mesh):
    in_specs = (
        P("seq", None),
        P("seq", "mp"),
        P("seq", None),
        P("seq", None),
        P("seq", "mp"),
        P("mp"),
        P("mp"),
        P("mp"),
        P("seq", "mp"),
    )
    out_specs = (P("seq", "mp"), P("seq", "mp"), P("mp"), P("mp"), P("mp"))
    return jax.shard_map(
        on_device, mesh=mesh, in_specs=in_specs, out_specs=out_specs, check_vma=False
    )
```
